32 devices in a mesh: pool: 4 (over y, x), slab: 8 (over z, core).
Axes of the slice: x: 2, y: 2, z: 4, core: 2. Of those that a mesh axis runs over, the one named last changes fastest.
Arguments:
- wave_coeff: bfloat16 [32, 2, 96, 9216], P(('pool', 'slab')), may hold values from -6 to 6
- response_coeff: bfloat16 [32, 2, 96, 9216], P(('pool', 'slab')), may hold values from -6 to 6
- band_index: int32 [32], P(('pool', 'slab')), may hold values from 0 to 31, each once
- occupation: int32 [32], replicated, may hold values from 0 to 2
- local_kernel: float32 [96, 9216], P('slab'), may hold values from 0.5 to 4
- gradient_kernel: float32 [96, 9216], P('slab'), may hold values from 0.25 to 2.5
Outputs:
- induced_potential: float32 [96, 9216], P('slab', 'pool')
The draws below stay inside these ranges and needn't reach their ends.
Inputs may be any that keep to these rules, and one draw needn't show every extreme that they name: `band_index`: a permutation of the 32 band numbers.
All inputs are finite; a program needn't handle non-finite values.
Results may differ from the reference program's by a relative error of at most 0.0067.
Values sent between devices are 32-bit elements; how exact they have to be, the bound alone decides.
A program may use at most 128 MiB of HBM per device.

```python
import math
import jax
import jax.numpy as jnp
from jax import lax

NG = 96
BANDS = 32


def with_ends(entries, key, low, largest):
    longest = entries.shape.index(max(entries.shape))
    spots = []
    for shift in (0, 1):
        where = [jax.random.randint(jax.random.fold_in(key, axis), (), 0, length) for axis, length in enumerate(entries.shape)]
        where[longest] = (where[longest] + shift) % entries.shape[longest]
        spots.append(tuple(where))
    return entries.at[spots[0]].set(low).at[spots[1]].set(largest)


def shard_levels(key, dims, cuts, low, largest):
    factor_of = 1.0
    for axis_at, parts in cuts:
        heights = jax.random.uniform(jax.random.fold_in(jax.random.fold_in(key, 6), axis_at), (parts,), jnp.float32, low / len(cuts), largest / len(cuts))
        factor_of = factor_of * jnp.repeat(jnp.exp(heights), dims[axis_at] // parts).reshape((-1,) + (1,) * (len(dims) - 1 - axis_at))
    return factor_of


def gaussian(key, dims, deviation, reach, cuts=(), kind=jnp.bfloat16):
    drawn = jax.random.normal(key, dims, jnp.float32) * deviation
    if len(cuts) > 0:
        drawn = shard_levels(key, dims, cuts, -0.22, 0.18) * drawn
    return jnp.clip(drawn, min=-reach, max=reach).astype(kind)


def setup_inputs(seed: int = 0) -> dict:
    streams_of = jax.random.split(jax.random.key(seed), 7)
    wave_coeff = gaussian(streams_of[0], (BANDS, 2, NG, NG * NG), 1.0, 6.0, ((0, 32),))
    response_coeff = gaussian(streams_of[1], (BANDS, 2, NG, NG * NG), 1.0, 6.0, ((0, 32),))
    band_index = jax.random.permutation(streams_of[2], BANDS).astype(jnp.int32)
    occupation = with_ends(jax.random.randint(streams_of[3], (BANDS,), 0, 3), jax.random.fold_in(streams_of[3], 1), 0, 2).astype(jnp.int32)
    local_kernel = jnp.clip(jnp.exp(math.log(4.0) - 2.0794415 * jax.random.uniform(streams_of[4], (NG, NG * NG), jnp.float32) ** shard_levels(streams_of[4], (NG, NG * NG), ((0, 8),), -0.2, 0.2)), 0.5, 4.0)
    gradient_kernel = jnp.clip(jnp.exp(math.log(2.5) - 2.3025851 * jax.random.uniform(streams_of[5], (NG, NG * NG), jnp.float32) ** shard_levels(streams_of[5], (NG, NG * NG), ((0, 8),), -0.2, 0.2)), 0.25, 2.5)
    return {"wave_coeff": wave_coeff, "response_coeff": response_coeff, "band_index": band_index, "occupation": occupation, "local_kernel": local_kernel, "gradient_kernel": gradient_kernel}


full_turn = 2.0 * math.pi

def stacked_table(length, sign, dtype):
    indices = jnp.arange(length, dtype=jnp.int32)
    product = indices[:, None] * indices[None, :] % length
    angles = product.astype(jnp.float32) * (full_turn / length)
    factor = 1.0 / math.sqrt(length)
    cosine = jnp.cos(angles) * factor
    sine_part = jnp.sin(angles) * factor
    upper_half = jnp.stack([cosine, -sign * sine_part], axis=1)
    lower_half = jnp.stack([sign * sine_part, cosine], axis=1)
    return jnp.stack([upper_half, lower_half], axis=0).astype(dtype)

def signed_freq(length, first_wave, amount):
    waves = first_wave + jnp.arange(amount, dtype=jnp.int32)
    return jnp.where(2 * waves >= length, waves - length, waves).astype(jnp.float32)

def coulomb_kernel(length, starts, counts):
    first_freq = signed_freq(length, starts[0], counts[0])[:, None, None]
    second_freq = signed_freq(length, starts[1], counts[1])[None, :, None]
    third_freq = signed_freq(length, starts[2], counts[2])[None, None, :]
    squared = (full_turn / length) ** 2 * (first_freq * first_freq + second_freq * second_freq + third_freq * third_freq)
    nonzero = jnp.where(squared > 0, squared, 1.0)
    return jnp.where(squared > 0, full_turn / nonzero, 0.0)

def to_space(tables, coeffs):
    first_pass = jnp.einsum('rzsk,skxy->rzxy', tables, coeffs.astype(jnp.float32)).astype(jnp.bfloat16)
    first_pass = lax.optimization_barrier(first_pass)
    second_pass = jnp.einsum('rxsk,szky->rzxy', tables, first_pass.astype(jnp.float32)).astype(jnp.bfloat16)
    second_pass = lax.optimization_barrier(second_pass)
    return jnp.einsum('rysk,szxk->rzxy', tables, second_pass.astype(jnp.float32))

def central(values, which_axis):
    return (jnp.roll(values, -1, which_axis) - jnp.roll(values, 1, which_axis)) * 0.5

def reference(wave_coeff, response_coeff, band_index, occupation, local_kernel, gradient_kernel):
    length = wave_coeff.shape[2]
    band_total = wave_coeff.shape[0]
    tables = stacked_table(length, 1.0, jnp.bfloat16).astype(jnp.float32)
    weights = occupation[band_index].astype(jnp.float32)
    cube_shape = (2, length, length, length)

    def one_band(running, band_items):
        wave_part, response_part, weight = band_items
        wave_space = to_space(tables, wave_part.reshape(cube_shape))
        response_space = to_space(tables, response_part.reshape(cube_shape))
        intersection = wave_space[0] * response_space[0] + wave_space[1] * response_space[1]
        return (running + weight * intersection, None)
    running = lax.scan(one_band, jnp.zeros((length, length, length), jnp.float32), (wave_coeff, response_coeff, weights))[0]
    density = running / band_total
    spectrum = jnp.fft.fftn(density, norm='ortho')
    kernel = coulomb_kernel(length, (0, 0, 0), (length, length, length))
    hartree = jnp.real(jnp.fft.ifftn(spectrum * kernel, norm='ortho'))
    coefficient = gradient_kernel.reshape(length, length, length)
    divergence = central(coefficient * central(density, 0), 0)
    divergence = divergence + central(coefficient * central(density, 1), 1)
    divergence = divergence + central(coefficient * central(density, 2), 2)
    potential = hartree + local_kernel.reshape(length, length, length) * density - divergence
    return potential.reshape(length, length * length)
```

```python
import functools
import math

import jax
import jax.numpy as jnp
import numpy as np
from jax import lax
from jax.experimental import pallas as pl
from jax.experimental.pallas import tpu as pltpu
from jax.sharding import PartitionSpec as P

full_turn = 2.0 * math.pi
MESH = pl.DeviceIdType.MESH


def stacked_table(length, sign, dtype):
    indices = jnp.arange(length, dtype=jnp.int32)
    product = indices[:, None] * indices[None, :] % length
    angles = product.astype(jnp.float32) * (full_turn / length)
    factor = 1.0 / math.sqrt(length)
    cosine = jnp.cos(angles) * factor
    sine_part = jnp.sin(angles) * factor
    upper_half = jnp.stack([cosine, -sign * sine_part], axis=1)
    lower_half = jnp.stack([sign * sine_part, cosine], axis=1)
    return jnp.stack([upper_half, lower_half], axis=0).astype(dtype)


def signed_freq(length, first_wave, amount):
    waves = first_wave + jnp.arange(amount, dtype=jnp.int32)
    return jnp.where(2 * waves >= length, waves - length, waves).astype(jnp.float32)


def exact_pass(spec, tables, values):
    return jnp.einsum(
        spec, tables, values, precision=lax.Precision.HIGHEST, preferred_element_type=jnp.float32
    )


def half_pass(spec, tables, values):
    return jnp.einsum(spec, tables, values, preferred_element_type=jnp.float32)


def band_weights(band_index, occupation):
    numbers = jnp.arange(occupation.shape[0], dtype=jnp.int32)
    matches = band_index[:, None] == numbers[None, :]
    return jnp.sum(jnp.where(matches, occupation[None, :], 0), axis=1).astype(jnp.float32)


def weighted_intersection(wave_space, response_space, weights, factor):
    intersection = wave_space[:, 0] * response_space[:, 0] + wave_space[:, 1] * response_space[:, 1]
    return jnp.sum(weights[:, None, None, None] * intersection, axis=0) * factor


def wrapped_window(block, first_row, width):
    extended = jnp.concatenate([block[:, -2:], block, block[:, :2]], axis=1)
    return lax.dynamic_slice_in_dim(extended, first_row, width + 4, 1)


def band_density(wave_coeff, response_coeff, weights, factor, slab_count, pool_count):
    length = wave_coeff.shape[2]
    cube_shape = (wave_coeff.shape[0], 2, length, length, length)
    inverse_half = stacked_table(length, 1.0, jnp.bfloat16)

    def to_space(coeff):
        planes = half_pass("rzsk,bskxy->brzxy", inverse_half, coeff.reshape(cube_shape)).astype(
            jnp.bfloat16
        )
        rows = half_pass("rxsk,bszky->brzxy", inverse_half, planes).astype(jnp.bfloat16)
        return half_pass("rysk,bszxk->brzxy", inverse_half, rows)

    density = weighted_intersection(to_space(wave_coeff), to_space(response_coeff), weights, factor)
    density = density.reshape(
        slab_count, length // slab_count, pool_count, length // pool_count, length
    )
    return jnp.transpose(density, (0, 2, 1, 3, 4)).reshape(slab_count, pool_count, -1, length)


def block_order(slab_rank, chips):
    return [lax.rem(slab_rank // 2 + step, chips) for step in list(range(1, chips)) + [0]]


def greet(devices):
    barrier = pltpu.get_barrier_semaphore()
    for device in devices:
        pl.semaphore_signal(barrier, inc=1, device_id=device, device_id_type=MESH)
    pl.semaphore_wait(barrier, len(devices))


def reduce_kernel(pools, slabs, part, full, first, second, own, third, gathered, sems_a, sems_b, sems_c, sems_d):
    pool = lax.axis_index("pool")
    slab = lax.axis_index("slab")
    chips = slabs // 2
    core = lax.rem(slab, 2)
    chip = slab // 2
    twin = (pool, 2 * chip + 1 - core)
    mates = [(lax.rem(pool + d, pools), slab) for d in range(1, pools)]
    column = [(pool, 2 * lax.rem(chip + e, chips) + core) for e in range(1, chips)]
    greet([twin] + mates + column)
    order = block_order(slab, chips)
    swaps = []
    for i, t in enumerate(order):
        copy = pltpu.make_async_remote_copy(
            src_ref=part.at[2 * t + 1 - core],
            dst_ref=first.at[i],
            send_sem=sems_a.at[0, i],
            recv_sem=sems_a.at[1, i],
            device_id=twin,
            device_id_type=MESH,
        )
        copy.start()
        swaps.append(copy)
    spreads = []
    for i, t in enumerate(order):
        swaps[i].wait()
        for q in range(pools):
            first[i, q] = first[i, q] + part[2 * t + core, q]
        row = []
        for d in range(1, pools):
            copy = pltpu.make_async_remote_copy(
                src_ref=first.at[i, lax.rem(pool + d, pools)],
                dst_ref=second.at[i, d - 1],
                send_sem=sems_b.at[0, i, d - 1],
                recv_sem=sems_b.at[1, i, d - 1],
                device_id=mates[d - 1],
                device_id_type=MESH,
            )
            copy.start()
            row.append(copy)
        spreads.append(row)
    lifts = []
    for i in range(chips):
        total = first[i, pool]
        for d, copy in enumerate(spreads[i]):
            copy.wait()
            total = total + second[i, d]
        own[i] = total
        if i < chips - 1:
            copy = pltpu.make_async_remote_copy(
                src_ref=own.at[i],
                dst_ref=third.at[i],
                send_sem=sems_c.at[0, i],
                recv_sem=sems_c.at[1, i],
                device_id=column[i],
                device_id_type=MESH,
            )
            copy.start()
            lifts.append(copy)
    total = own[chips - 1]
    for i, copy in enumerate(lifts):
        copy.wait()
        total = total + third[i]
    gathered[0] = total
    sends = []
    for d in range(1, pools):
        copy = pltpu.make_async_remote_copy(
            src_ref=gathered.at[0],
            dst_ref=gathered.at[d],
            send_sem=sems_d.at[0, d - 1],
            recv_sem=sems_d.at[1, d - 1],
            device_id=mates[d - 1],
            device_id_type=MESH,
        )
        copy.start()
        sends.append(copy)
    full[pool] = total
    for d in range(1, pools):
        sends[d - 1].wait()
        full[lax.rem(pool + pools - d, pools)] = gathered[d]


def reduce_density(part):
    slabs, pools, rows, lanes = part.shape
    chips = slabs // 2
    vmem = pl.BlockSpec(memory_space=pltpu.VMEM)
    return pl.pallas_call(
        functools.partial(reduce_kernel, pools, slabs),
        out_shape=jax.ShapeDtypeStruct((pools, rows, lanes), jnp.float32),
        in_specs=[vmem],
        out_specs=vmem,
        scratch_shapes=[
            pltpu.VMEM((chips, pools, rows, lanes), jnp.float32),
            pltpu.VMEM((chips, pools - 1, rows, lanes), jnp.float32),
            pltpu.VMEM((chips, rows, lanes), jnp.float32),
            pltpu.VMEM((chips - 1, rows, lanes), jnp.float32),
            pltpu.VMEM((pools, rows, lanes), jnp.float32),
            pltpu.SemaphoreType.DMA((2, chips)),
            pltpu.SemaphoreType.DMA((2, chips, pools - 1)),
            pltpu.SemaphoreType.DMA((2, chips - 1)),
            pltpu.SemaphoreType.DMA((2, pools - 1)),
        ],
        compiler_params=pltpu.CompilerParams(
            collective_id=0, has_side_effects=True, vmem_limit_bytes=56 * 2**20
        ),
    )(part)


def high_dot(a, b):
    return lax.dot_general(
        a,
        b,
        (((1,), (0,)), ((), ())),
        precision=lax.Precision.HIGHEST,
        preferred_element_type=jnp.float32,
    )


def screen_kernel(
    pools, slabs, spec, ahead, back, coulomb, edges, full, halos,
    landed, turned, returned, gathered, sems_a, sems_b, sems_c, sems_d,
):
    pool = lax.axis_index("pool")
    slab = lax.axis_index("slab")
    mates = [(lax.rem(pool + d, pools), slab) for d in range(1, pools)]
    column = [(pool, lax.rem(slab + e, slabs)) for e in range(1, slabs)]
    greet(mates + column)
    hops = slabs - 1

    def send(src, dst, sems, i, device):
        copy = pltpu.make_async_remote_copy(
            src_ref=src,
            dst_ref=dst,
            send_sem=sems.at[0, i],
            recv_sem=sems.at[1, i],
            device_id=device,
            device_id_type=MESH,
        )
        copy.start()
        return copy

    copies = [
        send(spec.at[lax.rem(slab + e, slabs)], landed.at[slab], sems_a, e - 1, column[e - 1])
        for e in range(1, slabs)
    ]
    rims = [
        send(edges.at[0], halos.at[0], sems_d, 0, column[0]),
        send(edges.at[1], halos.at[1], sems_d, 1, column[hops - 1]),
    ]
    landed[slab] = spec[slab]
    for copy in copies:
        copy.wait()
    kxs, zp, lanes = spec.shape[1:]
    length = coulomb.shape[1]
    sign = jnp.where(lax.broadcasted_iota(jnp.int32, (1, lanes), 1) < lanes // 2, 1.0, -1.0)
    for j in range(kxs):
        values = landed[:, j].reshape(slabs * zp, lanes)
        out = high_dot(ahead[...], values)
        mixed = out[:length] + sign * pltpu.roll(out[length:], lanes // 2, 1)
        mixed = mixed * coulomb[j]
        out = high_dot(back[...], mixed)
        half = slabs * zp
        mixed = out[:half] - sign * pltpu.roll(out[half:], lanes // 2, 1)
        turned[:, j] = mixed.reshape(slabs, zp, lanes)
    copies = [
        send(turned.at[lax.rem(slab + e, slabs)], returned.at[slab], sems_b, e - 1, column[e - 1])
        for e in range(1, slabs)
    ]
    returned[slab] = turned[slab]
    for copy in copies:
        copy.wait()
    copies = [
        send(returned, gathered.at[d - 1], sems_c, d - 1, mates[d - 1]) for d in range(1, pools)
    ]
    full[pool] = returned[...]
    for d in range(1, pools):
        copies[d - 1].wait()
        full[lax.rem(pool + pools - d, pools)] = gathered[d - 1]
    for copy in rims:
        copy.wait()


def screened(spec, ahead, back, coulomb, edges, pools):
    slabs, kxs, zp, lanes = spec.shape
    vmem = pl.BlockSpec(memory_space=pltpu.VMEM)
    return pl.pallas_call(
        functools.partial(screen_kernel, pools, slabs),
        out_shape=(
            jax.ShapeDtypeStruct((pools, slabs, kxs, zp, lanes), jnp.float32),
            jax.ShapeDtypeStruct(edges.shape, jnp.float32),
        ),
        in_specs=[vmem] * 5,
        out_specs=(vmem, vmem),
        scratch_shapes=[
            pltpu.VMEM((slabs, kxs, zp, lanes), jnp.float32),
            pltpu.VMEM((slabs, kxs, zp, lanes), jnp.float32),
            pltpu.VMEM((slabs, kxs, zp, lanes), jnp.float32),
            pltpu.VMEM((pools - 1, slabs, kxs, zp, lanes), jnp.float32),
            pltpu.SemaphoreType.DMA((2, slabs - 1)),
            pltpu.SemaphoreType.DMA((2, slabs - 1)),
            pltpu.SemaphoreType.DMA((2, pools - 1)),
            pltpu.SemaphoreType.DMA((2, 2)),
        ],
        compiler_params=pltpu.CompilerParams(
            collective_id=1, has_side_effects=True, vmem_limit_bytes=40 * 2**20
        ),
    )(spec, ahead, back, coulomb, edges)


def waves(length):
    index = np.arange(length)
    angle = (index[:, None] * index[None, :] % length) * (full_turn / length)
    return np.cos(angle) / math.sqrt(length), np.sin(angle) / math.sqrt(length)


def hartree_tables(length, pools, slabs):
    cosine, sine = waves(length)
    planes, kxn = length // slabs, length // pools
    zp = -(-planes // 8) * 8
    kxs = -(-kxn // slabs)
    padded = kxs * slabs
    half = length // 2 + 1
    lanes = 128
    mid = lanes // 2
    y_ahead = np.zeros((length, lanes))
    y_ahead[:, :half] = cosine[:, :half]
    y_ahead[:, mid : mid + half] = -sine[:, :half]
    weight = np.full((half, 1), 2.0)
    weight[0] = 1.0
    if length % 2 == 0:
        weight[-1] = 1.0
    y_back = np.zeros((lanes, length))
    y_back[:half] = weight * cosine[:half]
    y_back[mid : mid + half] = -weight * sine[:half]
    x_ahead = np.zeros((pools, 2, padded, length))
    x_back = np.zeros((pools, 2, kxn, pools, padded))
    for r, table in enumerate((cosine, sine)):
        x_ahead[:, r, :kxn] = table.reshape(pools, kxn, length)
        x_back[:, r, :, :, :kxn] = table.reshape(pools, kxn, pools, kxn)
    z_ahead = np.zeros((2, length, slabs, zp))
    z_back = np.zeros((2, slabs, zp, length))
    for r, table in enumerate((cosine, sine)):
        z_ahead[r, :, :, :planes] = table.reshape(length, slabs, planes)
        z_back[r, :, :planes] = table.reshape(slabs, planes, length)
    z_ahead = z_ahead.reshape(2 * length, slabs * zp)
    z_back = z_back.reshape(2 * slabs * zp, length)
    tables = (y_ahead, y_back, x_ahead, x_back, z_ahead, z_back)
    return [jnp.asarray(t.astype(np.float32)) for t in tables]


def shards(wave_coeff, response_coeff, band_index, occupation, local_kernel, gradient_kernel):
    length = wave_coeff.shape[2]
    band_count = wave_coeff.shape[0]
    slab_count = lax.axis_size("slab")
    pool_count = lax.axis_size("pool")
    planes = length // slab_count
    columns = length // pool_count
    slab_rank = lax.axis_index("slab")
    pool_rank = lax.axis_index("pool")
    first_row = pool_rank * columns
    factor = 1.0 / occupation.shape[0]
    y_ahead, y_back, x_ahead, x_back, z_ahead, z_back = hartree_tables(
        length, pool_count, slab_count
    )
    weights = band_weights(band_index, occupation)
    part = band_density(wave_coeff, response_coeff, weights, factor, slab_count, pool_count)
    blocks = reduce_density(part).reshape(pool_count, planes, columns, length)

    lanes = y_ahead.shape[1]
    sign = jnp.where(jnp.arange(lanes) < lanes // 2, 1.0, -1.0).astype(jnp.float32)
    along = exact_pass("qzxy,yl->qzxl", blocks, y_ahead)
    turn = x_ahead[pool_rank].reshape(2, -1, pool_count, columns)
    both = exact_pass("rkqx,qzxl->rkzl", turn, along)
    spec = both[0] + sign * jnp.roll(both[1], lanes // 2, 2)
    zp = z_ahead.shape[1] // slab_count
    kxs = spec.shape[0] // slab_count
    spec = jnp.pad(spec, ((0, 0), (0, zp - planes), (0, 0)))
    spec = spec.reshape(slab_count, kxs, zp, lanes)
    kx = signed_freq(length, pool_rank * columns + slab_rank * kxs, kxs)[:, None, None]
    kz = signed_freq(length, 0, length)[None, :, None]
    ky = (jnp.arange(lanes) % (lanes // 2)).astype(jnp.float32)[None, None, :]
    squared = (full_turn / length) ** 2 * (kz * kz + kx * kx + ky * ky)
    coulomb = jnp.where(squared > 0, full_turn / jnp.where(squared > 0, squared, 1.0), 0.0)

    interior = blocks[pool_rank]
    gradient = gradient_kernel.reshape(planes, length, length)
    gradient_own = lax.dynamic_slice_in_dim(gradient, first_row, columns, 1)
    edges = jnp.stack(
        [
            jnp.concatenate([interior[-2:], gradient_own[-1:]]),
            jnp.concatenate([interior[:2], gradient_own[:1]]),
        ]
    )
    returned, halos = screened(spec, z_ahead, z_back, coulomb, edges, pool_count)

    tall = jnp.concatenate([halos[0, :2], interior, halos[1, :2]], axis=0)
    tall_gradient = jnp.concatenate([halos[0, 2:], gradient_own, halos[1, 2:]], axis=0)
    depth_flux = tall_gradient * ((tall[2:] - tall[:-2]) * 0.5)
    depth_div = (depth_flux[2:] - depth_flux[:-2]) * 0.5
    slab_density = jnp.transpose(blocks, (1, 0, 2, 3)).reshape(planes, length, length)
    wide = wrapped_window(slab_density, first_row, columns)
    wide_gradient = wrapped_window(gradient, first_row, columns)[:, 1:-1]
    across_flux = wide_gradient * ((wide[:, 2:] - wide[:, :-2]) * 0.5)
    across_div = (across_flux[:, 2:] - across_flux[:, :-2]) * 0.5
    along_flux = gradient_own * ((jnp.roll(interior, -1, 2) - jnp.roll(interior, 1, 2)) * 0.5)
    along_div = (jnp.roll(along_flux, -1, 2) - jnp.roll(along_flux, 1, 2)) * 0.5
    local_block = lax.dynamic_slice_in_dim(
        local_kernel.reshape(planes, length, length), first_row, columns, 1
    )
    rest = local_block * interior - (depth_div + across_div + along_div)

    returned = returned.reshape(pool_count, kxs * slab_count, zp, lanes)[:, :, :planes]
    both = exact_pass("rxpk,pkzl->rzxl", x_back[pool_rank], returned)
    across = both[0] - sign * jnp.roll(both[1], lanes // 2, 2)
    potential = exact_pass("zxl,ly->zxy", across, y_back) + rest
    return potential.reshape(planes, columns * length)


def solution(mesh):
    return jax.shard_map(
        shards,
        mesh=mesh,
        in_specs=(
            P(("pool", "slab"), None, None, None),
            P(("pool", "slab"), None, None, None),
            P(("pool", "slab")),
            P(),
            P("slab", None),
            P("slab", None),
        ),
        out_specs=P("slab", "pool"),
        check_vma=False,
    )
```

```python
import functools
import math

import jax
import jax.numpy as jnp
import numpy as np
from jax import lax
from jax.experimental import pallas as pl
from jax.experimental.pallas import tpu as pltpu
from jax.sharding import PartitionSpec as P

full_turn = 2.0 * math.pi
MESH = pl.DeviceIdType.MESH


def stacked_table(length, sign, dtype):
    indices = jnp.arange(length, dtype=jnp.int32)
    product = indices[:, None] * indices[None, :] % length
    angles = product.astype(jnp.float32) * (full_turn / length)
    factor = 1.0 / math.sqrt(length)
    cosine = jnp.cos(angles) * factor
    sine_part = jnp.sin(angles) * factor
    upper_half = jnp.stack([cosine, -sign * sine_part], axis=1)
    lower_half = jnp.stack([sign * sine_part, cosine], axis=1)
    return jnp.stack([upper_half, lower_half], axis=0).astype(dtype)


def signed_freq(length, first_wave, amount):
    waves = first_wave + jnp.arange(amount, dtype=jnp.int32)
    return jnp.where(2 * waves >= length, waves - length, waves).astype(jnp.float32)


def exact_pass(spec, tables, values):
    return jnp.einsum(
        spec, tables, values, precision=lax.Precision.HIGHEST, preferred_element_type=jnp.float32
    )


def band_weights(band_index, occupation):
    numbers = jnp.arange(occupation.shape[0], dtype=jnp.int32)
    matches = band_index[:, None] == numbers[None, :]
    return jnp.sum(jnp.where(matches, occupation[None, :], 0), axis=1).astype(jnp.float32)


def wrapped_window(block, first_row, width):
    extended = jnp.concatenate([block[:, -2:], block, block[:, :2]], axis=1)
    return lax.dynamic_slice_in_dim(extended, first_row, width + 4, 1)


def band_kernel(bands, length, weight, wave, response, table, y_re, y_im, density, wave_cols, response_cols):
    chunk = math.lcm(length, 128)
    per = chunk // length
    twice = 2 * length

    def one_dot(a, b):
        return jnp.dot(a, b, preferred_element_type=jnp.float32)

    for b in range(bands):
        for source, target in ((wave, wave_cols), (response, response_cols)):

            def depth_step(c, carry, source=source, target=target):
                start = pl.multiple_of(c * chunk, 128)
                out = one_dot(table[...], source[b, :, pl.ds(start, chunk)])
                for m in range(per):
                    row = pl.multiple_of((c * per + m) * twice, 8)
                    target[pl.ds(row, twice), 0:length] = out[:, m * length : (m + 1) * length]
                return carry

            lax.fori_loop(0, length * length // chunk, depth_step, 0, unroll=2)

        def space(target, z):
            pieces = []
            for k in (0, 1):
                halves = [
                    target[pl.ds(z + k + s * length, length, stride=twice), :] for s in (0, 1)
                ]
                pieces.append(jnp.concatenate(halves, axis=0))
            values = jnp.concatenate(pieces, axis=1).astype(jnp.bfloat16)
            rows = one_dot(table[...], values).astype(jnp.bfloat16)
            lanes = target.shape[1]
            re, im = (
                jnp.concatenate(
                    [rows[r * length : (r + 1) * length, k * lanes : k * lanes + length] for k in (0, 1)],
                    axis=0,
                )
                for r in (0, 1)
            )
            return one_dot(re, y_re[...]) + one_dot(im, y_im[...])

        def plane_step(i, carry):
            z = 2 * i
            product = space(wave_cols, z) * space(response_cols, z)
            half = product.shape[1] // 2
            value = (product[:, :length] + product[:, half : half + length]) * weight[b]
            for k in (0, 1):
                part = value[k * length : (k + 1) * length]
                density[z + k] = part if b == 0 else density[z + k] + part
            return carry

        lax.fori_loop(0, length // 2, plane_step, 0, unroll=2)


def band_density(wave_coeff, response_coeff, weights, factor, slab_count, pool_count):
    bands, _, length, flat = wave_coeff.shape
    shape = (bands, 2 * length, flat)
    full = stacked_table(length, 1.0, jnp.bfloat16)
    table = full.reshape(2 * length, 2 * length)
    lanes = -(-length // 128) * 128
    sides = ((0, 0), (0, lanes - length))
    y_re = jnp.concatenate([jnp.pad(full[r, :, 0].T, sides) for r in (0, 1)], axis=1)
    y_im = jnp.concatenate([jnp.pad(full[r, :, 1].T, sides) for r in (0, 1)], axis=1)
    vmem = pl.BlockSpec(memory_space=pltpu.VMEM)
    density = pl.pallas_call(
        functools.partial(band_kernel, bands, length),
        out_shape=jax.ShapeDtypeStruct((length, length, length), jnp.float32),
        in_specs=[pl.BlockSpec(memory_space=pltpu.SMEM)] + [vmem] * 5,
        out_specs=vmem,
        scratch_shapes=[pltpu.VMEM((2 * length * length, lanes), jnp.float32)] * 2,
        compiler_params=pltpu.CompilerParams(vmem_limit_bytes=48 * 2**20),
    )(weights * factor, wave_coeff.reshape(shape), response_coeff.reshape(shape), table, y_re, y_im)
    density = density.reshape(
        slab_count, length // slab_count, pool_count, length // pool_count, length
    )
    return jnp.transpose(density, (0, 2, 1, 3, 4)).reshape(slab_count, pool_count, -1, length)


def block_order(slab_rank, chips):
    return [lax.rem(slab_rank // 2 + step, chips) for step in list(range(1, chips)) + [0]]


def greet(devices):
    barrier = pltpu.get_barrier_semaphore()
    for device in devices:
        pl.semaphore_signal(barrier, inc=1, device_id=device, device_id_type=MESH)
    pl.semaphore_wait(barrier, len(devices))


def reduce_kernel(pools, slabs, part, full, first, second, own, third, gathered, sems_a, sems_b, sems_c, sems_d):
    pool = lax.axis_index("pool")
    slab = lax.axis_index("slab")
    chips = slabs // 2
    core = lax.rem(slab, 2)
    chip = slab // 2
    twin = (pool, 2 * chip + 1 - core)
    mates = [(lax.rem(pool + d, pools), slab) for d in range(1, pools)]
    column = [(pool, 2 * lax.rem(chip + e, chips) + core) for e in range(1, chips)]
    greet([twin] + mates + column)
    order = block_order(slab, chips)
    swaps = []
    for i, t in enumerate(order):
        copy = pltpu.make_async_remote_copy(
            src_ref=part.at[2 * t + 1 - core],
            dst_ref=first.at[i],
            send_sem=sems_a.at[0, i],
            recv_sem=sems_a.at[1, i],
            device_id=twin,
            device_id_type=MESH,
        )
        copy.start()
        swaps.append(copy)
    spreads = []
    for i, t in enumerate(order):
        swaps[i].wait()
        for q in range(pools):
            first[i, q] = first[i, q] + part[2 * t + core, q]
        row = []
        for d in range(1, pools):
            copy = pltpu.make_async_remote_copy(
                src_ref=first.at[i, lax.rem(pool + d, pools)],
                dst_ref=second.at[i, d - 1],
                send_sem=sems_b.at[0, i, d - 1],
                recv_sem=sems_b.at[1, i, d - 1],
                device_id=mates[d - 1],
                device_id_type=MESH,
            )
            copy.start()
            row.append(copy)
        spreads.append(row)
    lifts = []
    for i in range(chips):
        total = first[i, pool]
        for d, copy in enumerate(spreads[i]):
            copy.wait()
            total = total + second[i, d]
        own[i] = total
        if i < chips - 1:
            copy = pltpu.make_async_remote_copy(
                src_ref=own.at[i],
                dst_ref=third.at[i],
                send_sem=sems_c.at[0, i],
                recv_sem=sems_c.at[1, i],
                device_id=column[i],
                device_id_type=MESH,
            )
            copy.start()
            lifts.append(copy)
    total = own[chips - 1]
    for i, copy in enumerate(lifts):
        copy.wait()
        total = total + third[i]
    gathered[0] = total
    sends = []
    for d in range(1, pools):
        copy = pltpu.make_async_remote_copy(
            src_ref=gathered.at[0],
            dst_ref=gathered.at[d],
            send_sem=sems_d.at[0, d - 1],
            recv_sem=sems_d.at[1, d - 1],
            device_id=mates[d - 1],
            device_id_type=MESH,
        )
        copy.start()
        sends.append(copy)
    full[pool] = total
    for d in range(1, pools):
        sends[d - 1].wait()
        full[lax.rem(pool + pools - d, pools)] = gathered[d]


def reduce_density(part):
    slabs, pools, rows, lanes = part.shape
    chips = slabs // 2
    vmem = pl.BlockSpec(memory_space=pltpu.VMEM)
    return pl.pallas_call(
        functools.partial(reduce_kernel, pools, slabs),
        out_shape=jax.ShapeDtypeStruct((pools, rows, lanes), jnp.float32),
        in_specs=[vmem],
        out_specs=vmem,
        scratch_shapes=[
            pltpu.VMEM((chips, pools, rows, lanes), jnp.float32),
            pltpu.VMEM((chips, pools - 1, rows, lanes), jnp.float32),
            pltpu.VMEM((chips, rows, lanes), jnp.float32),
            pltpu.VMEM((chips - 1, rows, lanes), jnp.float32),
            pltpu.VMEM((pools, rows, lanes), jnp.float32),
            pltpu.SemaphoreType.DMA((2, chips)),
            pltpu.SemaphoreType.DMA((2, chips, pools - 1)),
            pltpu.SemaphoreType.DMA((2, chips - 1)),
            pltpu.SemaphoreType.DMA((2, pools - 1)),
        ],
        compiler_params=pltpu.CompilerParams(
            collective_id=0, has_side_effects=True, vmem_limit_bytes=56 * 2**20
        ),
    )(part)


def high_dot(a, b):
    return lax.dot_general(
        a,
        b,
        (((1,), (0,)), ((), ())),
        precision=lax.Precision.HIGHEST,
        preferred_element_type=jnp.float32,
    )


def screen_kernel(
    pools, slabs, spec, ahead, back, coulomb, edges, full, halos,
    landed, turned, returned, gathered, sems_a, sems_b, sems_c, sems_d,
):
    pool = lax.axis_index("pool")
    slab = lax.axis_index("slab")
    mates = [(lax.rem(pool + d, pools), slab) for d in range(1, pools)]
    column = [(pool, lax.rem(slab + e, slabs)) for e in range(1, slabs)]
    greet(mates + column)
    hops = slabs - 1

    def send(src, dst, sems, i, device):
        copy = pltpu.make_async_remote_copy(
            src_ref=src,
            dst_ref=dst,
            send_sem=sems.at[0, i],
            recv_sem=sems.at[1, i],
            device_id=device,
            device_id_type=MESH,
        )
        copy.start()
        return copy

    copies = [
        send(spec.at[lax.rem(slab + e, slabs)], landed.at[slab], sems_a, e - 1, column[e - 1])
        for e in range(1, slabs)
    ]
    rims = [
        send(edges.at[0], halos.at[0], sems_d, 0, column[0]),
        send(edges.at[1], halos.at[1], sems_d, 1, column[hops - 1]),
    ]
    landed[slab] = spec[slab]
    for copy in copies:
        copy.wait()
    kxs, zp, lanes = spec.shape[1:]
    length = coulomb.shape[1]
    sign = jnp.where(lax.broadcasted_iota(jnp.int32, (1, lanes), 1) < lanes // 2, 1.0, -1.0)
    for j in range(kxs):
        values = landed[:, j].reshape(slabs * zp, lanes)
        out = high_dot(ahead[...], values)
        mixed = out[:length] + sign * pltpu.roll(out[length:], lanes // 2, 1)
        mixed = mixed * coulomb[j]
        out = high_dot(back[...], mixed)
        half = slabs * zp
        mixed = out[:half] - sign * pltpu.roll(out[half:], lanes // 2, 1)
        turned[:, j] = mixed.reshape(slabs, zp, lanes)
    copies = [
        send(turned.at[lax.rem(slab + e, slabs)], returned.at[slab], sems_b, e - 1, column[e - 1])
        for e in range(1, slabs)
    ]
    returned[slab] = turned[slab]
    for copy in copies:
        copy.wait()
    copies = [
        send(returned, gathered.at[d - 1], sems_c, d - 1, mates[d - 1]) for d in range(1, pools)
    ]
    full[pool] = returned[...]
    for d in range(1, pools):
        copies[d - 1].wait()
        full[lax.rem(pool + pools - d, pools)] = gathered[d - 1]
    for copy in rims:
        copy.wait()


def screened(spec, ahead, back, coulomb, edges, pools):
    slabs, kxs, zp, lanes = spec.shape
    vmem = pl.BlockSpec(memory_space=pltpu.VMEM)
    return pl.pallas_call(
        functools.partial(screen_kernel, pools, slabs),
        out_shape=(
            jax.ShapeDtypeStruct((pools, slabs, kxs, zp, lanes), jnp.float32),
            jax.ShapeDtypeStruct(edges.shape, jnp.float32),
        ),
        in_specs=[vmem] * 5,
        out_specs=(vmem, vmem),
        scratch_shapes=[
            pltpu.VMEM((slabs, kxs, zp, lanes), jnp.float32),
            pltpu.VMEM((slabs, kxs, zp, lanes), jnp.float32),
            pltpu.VMEM((slabs, kxs, zp, lanes), jnp.float32),
            pltpu.VMEM((pools - 1, slabs, kxs, zp, lanes), jnp.float32),
            pltpu.SemaphoreType.DMA((2, slabs - 1)),
            pltpu.SemaphoreType.DMA((2, slabs - 1)),
            pltpu.SemaphoreType.DMA((2, pools - 1)),
            pltpu.SemaphoreType.DMA((2, 2)),
        ],
        compiler_params=pltpu.CompilerParams(
            collective_id=1, has_side_effects=True, vmem_limit_bytes=40 * 2**20
        ),
    )(spec, ahead, back, coulomb, edges)


def waves(length):
    index = np.arange(length)
    angle = (index[:, None] * index[None, :] % length) * (full_turn / length)
    return np.cos(angle) / math.sqrt(length), np.sin(angle) / math.sqrt(length)


def hartree_tables(length, pools, slabs):
    cosine, sine = waves(length)
    planes, kxn = length // slabs, length // pools
    zp = -(-planes // 8) * 8
    kxs = -(-kxn // slabs)
    padded = kxs * slabs
    half = length // 2 + 1
    lanes = 128
    mid = lanes // 2
    y_ahead = np.zeros((length, lanes))
    y_ahead[:, :half] = cosine[:, :half]
    y_ahead[:, mid : mid + half] = -sine[:, :half]
    weight = np.full((half, 1), 2.0)
    weight[0] = 1.0
    if length % 2 == 0:
        weight[-1] = 1.0
    y_back = np.zeros((lanes, length))
    y_back[:half] = weight * cosine[:half]
    y_back[mid : mid + half] = -weight * sine[:half]
    x_ahead = np.zeros((pools, 2, padded, length))
    x_back = np.zeros((pools, 2, kxn, pools, padded))
    for r, table in enumerate((cosine, sine)):
        x_ahead[:, r, :kxn] = table.reshape(pools, kxn, length)
        x_back[:, r, :, :, :kxn] = table.reshape(pools, kxn, pools, kxn)
    z_ahead = np.zeros((2, length, slabs, zp))
    z_back = np.zeros((2, slabs, zp, length))
    for r, table in enumerate((cosine, sine)):
        z_ahead[r, :, :, :planes] = table.reshape(length, slabs, planes)
        z_back[r, :, :planes] = table.reshape(slabs, planes, length)
    z_ahead = z_ahead.reshape(2 * length, slabs * zp)
    z_back = z_back.reshape(2 * slabs * zp, length)
    tables = (y_ahead, y_back, x_ahead, x_back, z_ahead, z_back)
    return [jnp.asarray(t.astype(np.float32)) for t in tables]


def shards(wave_coeff, response_coeff, band_index, occupation, local_kernel, gradient_kernel):
    length = wave_coeff.shape[2]
    band_count = wave_coeff.shape[0]
    slab_count = lax.axis_size("slab")
    pool_count = lax.axis_size("pool")
    planes = length // slab_count
    columns = length // pool_count
    slab_rank = lax.axis_index("slab")
    pool_rank = lax.axis_index("pool")
    first_row = pool_rank * columns
    factor = 1.0 / occupation.shape[0]
    y_ahead, y_back, x_ahead, x_back, z_ahead, z_back = hartree_tables(
        length, pool_count, slab_count
    )
    weights = band_weights(band_index, occupation)
    part = band_density(wave_coeff, response_coeff, weights, factor, slab_count, pool_count)
    blocks = reduce_density(part).reshape(pool_count, planes, columns, length)

    lanes = y_ahead.shape[1]
    sign = jnp.where(jnp.arange(lanes) < lanes // 2, 1.0, -1.0).astype(jnp.float32)
    along = exact_pass("qzxy,yl->qzxl", blocks, y_ahead)
    turn = x_ahead[pool_rank].reshape(2, -1, pool_count, columns)
    both = exact_pass("rkqx,qzxl->rkzl", turn, along)
    spec = both[0] + sign * jnp.roll(both[1], lanes // 2, 2)
    zp = z_ahead.shape[1] // slab_count
    kxs = spec.shape[0] // slab_count
    spec = jnp.pad(spec, ((0, 0), (0, zp - planes), (0, 0)))
    spec = spec.reshape(slab_count, kxs, zp, lanes)
    kx = signed_freq(length, pool_rank * columns + slab_rank * kxs, kxs)[:, None, None]
    kz = signed_freq(length, 0, length)[None, :, None]
    ky = (jnp.arange(lanes) % (lanes // 2)).astype(jnp.float32)[None, None, :]
    squared = (full_turn / length) ** 2 * (kz * kz + kx * kx + ky * ky)
    coulomb = jnp.where(squared > 0, full_turn / jnp.where(squared > 0, squared, 1.0), 0.0)

    interior = blocks[pool_rank]
    gradient = gradient_kernel.reshape(planes, length, length)
    gradient_own = lax.dynamic_slice_in_dim(gradient, first_row, columns, 1)
    edges = jnp.stack(
        [
            jnp.concatenate([interior[-2:], gradient_own[-1:]]),
            jnp.concatenate([interior[:2], gradient_own[:1]]),
        ]
    )
    returned, halos = screened(spec, z_ahead, z_back, coulomb, edges, pool_count)

    tall = jnp.concatenate([halos[0, :2], interior, halos[1, :2]], axis=0)
    tall_gradient = jnp.concatenate([halos[0, 2:], gradient_own, halos[1, 2:]], axis=0)
    depth_flux = tall_gradient * ((tall[2:] - tall[:-2]) * 0.5)
    depth_div = (depth_flux[2:] - depth_flux[:-2]) * 0.5
    slab_density = jnp.transpose(blocks, (1, 0, 2, 3)).reshape(planes, length, length)
    wide = wrapped_window(slab_density, first_row, columns)
    wide_gradient = wrapped_window(gradient, first_row, columns)[:, 1:-1]
    across_flux = wide_gradient * ((wide[:, 2:] - wide[:, :-2]) * 0.5)
    across_div = (across_flux[:, 2:] - across_flux[:, :-2]) * 0.5
    along_flux = gradient_own * ((jnp.roll(interior, -1, 2) - jnp.roll(interior, 1, 2)) * 0.5)
    along_div = (jnp.roll(along_flux, -1, 2) - jnp.roll(along_flux, 1, 2)) * 0.5
    local_block = lax.dynamic_slice_in_dim(
        local_kernel.reshape(planes, length, length), first_row, columns, 1
    )
    rest = local_block * interior - (depth_div + across_div + along_div)

    returned = returned.reshape(pool_count, kxs * slab_count, zp, lanes)[:, :, :planes]
    both = exact_pass("rxpk,pkzl->rzxl", x_back[pool_rank], returned)
    across = both[0] - sign * jnp.roll(both[1], lanes // 2, 2)
    potential = exact_pass("zxl,ly->zxy", across, y_back) + rest
    return potential.reshape(planes, columns * length)


def solution(mesh):
    return jax.shard_map(
        shards,
        mesh=mesh,
        in_specs=(
            P(("pool", "slab"), None, None, None),
            P(("pool", "slab"), None, None, None),
            P(("pool", "slab")),
            P(),
            P("slab", None),
            P("slab", None),
        ),
        out_specs=P("slab", "pool"),
        check_vma=False,
    )
```
